8 devices in a mesh: dp: 2 (over y, z), sp: 4 (over x, core).
Axes of the slice: x: 2, y: 2, z: 1, core: 2. Of those that a mesh axis runs over, the one named last changes fastest.
Arguments:
- q: bfloat16 [64, 96, 192], P('dp'), parts along dimension 0
- k: bfloat16 [64, 8192, 8, 192], P('dp', 'sp'), parts along dimension 0
- v: bfloat16 [64, 8192, 8, 192], P('dp', 'sp'), parts along dimension 0
Outputs:
- q: bfloat16 [64, 96, 192], P('dp'), parts along dimension 0
There are 2 independent parts. The reference program is written for one: setup_inputs(seed, part) draws one part's arguments, and reference() takes and returns one part's arrays. A program takes and returns all parts, laid end to end along the dimension named above; each array names one.
All inputs are finite; a program needn't handle non-finite values.
Results may differ from the reference program's by a relative error of at most 0.012.
Values are sent between devices in bfloat16 or wider.
A program may use at most 2 GiB of HBM per device.

```python
import jax
import jax.numpy as jnp

BATCH = 32
CACHE = 8192
HEADS = 96
KV_HEADS = 8
HEAD = 192


def setup_inputs(seed: int = 0, part: int = 0) -> dict:
    kq, kk, kv = (jax.random.fold_in(k, part) for k in jax.random.split(jax.random.key(seed), 3))
    return {
        "q": (3 * jax.random.normal(kq, (BATCH, HEADS, HEAD), jnp.float32)).astype(jnp.bfloat16),
        "k": jax.random.normal(kk, (BATCH, CACHE, KV_HEADS, HEAD), jnp.float32).astype(jnp.bfloat16),
        "v": jax.random.normal(kv, (BATCH, CACHE, KV_HEADS, HEAD), jnp.float32).astype(jnp.bfloat16),
    }


def einsum(form, a, b):
    return jnp.einsum(form, a.astype(jnp.float32), b.astype(jnp.float32))


def reference(q, k, v):
    grouped = q.reshape(BATCH, KV_HEADS, -1, HEAD)
    scores = einsum("bgsd,bugd->bgsu", grouped, k) * HEAD**-0.5
    weights = jax.nn.softmax(scores, -1).astype(jnp.bfloat16)
    return einsum("bgsu,bugd->bgsd", weights, v).astype(jnp.bfloat16).reshape(BATCH, HEADS, HEAD)
```

```python
import functools

import jax
import jax.numpy as jnp
from jax import lax
from jax.experimental import pallas as pl
from jax.experimental.pallas import tpu as pltpu
from jax.sharding import PartitionSpec as P

GROUP = 4
SLOTS = 4
LAG = 3
LOG2E = 1.4426950408889634


def kernel(ranks, q_hbm, k_hbm, v_hbm, out, keys, values, queries, whole, seen, parts, stats, scales, sems, q_sem, part_send, part_recv, stat_send, stat_recv):
    me = lax.axis_index("sp")
    sequences, heads, head = q_hbm.shape
    kv_heads = k_hbm.shape[0] // sequences
    each = heads // kv_heads
    per = kv_heads // GROUP
    units = sequences * per
    factor = head**-0.5 * LOG2E
    others = [lax.rem(me + d, ranks) for d in range(1, ranks)]

    def fetch(unit, slot, source, target, row):
        return pltpu.make_async_copy(source.at[pl.ds(unit * GROUP, GROUP)], target.at[slot], sems.at[row, slot])

    def fetch_k(unit, slot):
        return fetch(unit, slot, k_hbm, keys, 0)

    def fetch_v(unit, slot):
        return fetch(unit, slot, v_hbm, values, 1)

    q_copy = pltpu.make_async_copy(q_hbm, queries, q_sem)
    q_copy.start()
    for unit in range(SLOTS):
        fetch_k(unit, unit).start()
        fetch_v(unit, unit).start()

    barrier = pltpu.get_barrier_semaphore()
    for other in others:
        pl.semaphore_signal(barrier, inc=1, device_id={"sp": other})
    pl.semaphore_wait(barrier, ranks - 1)
    whole[...] = jnp.zeros_like(whole)
    q_copy.wait()

    def send(buffer, owner, b, to, send_sem, recv_sem):
        place = buffer.at[owner, b]
        return pltpu.make_async_remote_copy(place, place, send_sem, recv_sem.at[owner, b], device_id={"sp": to})

    def sends(b):
        for d, other in enumerate(others):
            yield send(parts, me, b, other, part_send.at[d, b], part_recv)
            yield send(stats, me, b, other, stat_send.at[d, b], stat_recv)

    def attend(b):
        whole[:heads] = queries[b].astype(jnp.float32)
        lane = lax.broadcasted_iota(jnp.int32, (16, 128), 1)
        stat = jnp.zeros((16, 128), jnp.float32)
        for group in range(per):
            unit = b * per + group
            slot = lax.rem(unit, SLOTS)
            fetch_k(unit, slot).wait()
            weights = []
            for g in range(GROUP):
                row = (group * GROUP + g) * each
                query = whole[row : row + 16].astype(jnp.bfloat16)
                scores = jnp.dot(query, keys[slot, g], preferred_element_type=jnp.float32)
                high = jnp.max(scores, -1, keepdims=True)
                weight = jnp.exp2((scores - high) * factor)
                total = jnp.sum(weight, -1, keepdims=True)
                stat = jnp.where(lane == group * GROUP + g, high, stat)
                stat = jnp.where(lane == 64 + group * GROUP + g, total, stat)
                weights.append(weight.astype(jnp.bfloat16))
            fetch_v(unit, slot).wait()
            for g in range(GROUP):
                row = (group * GROUP + g) * each
                result = lax.dot_general(weights[g], values[slot, g], (((1,), (1,)), ((), ())), preferred_element_type=jnp.float32)
                seen[row : row + each] = result[:each]

            @pl.when(unit + SLOTS < units)
            def _():
                fetch_k(unit + SLOTS, slot).start()
                fetch_v(unit + SLOTS, slot).start()

        parts[me, b] = seen[...].astype(jnp.bfloat16)
        stats[me, b] = stat
        for copy in sends(b):
            copy.start()

    def together(b):
        for other in others:
            send(parts, other, b, other, part_send.at[0, b], part_recv).wait_recv()
            send(stats, other, b, other, stat_send.at[0, b], stat_recv).wait_recv()
        stat = [stats[r, b] for r in range(ranks)]
        high = functools.reduce(jnp.maximum, stat)
        scale = [jnp.exp2((s - high) * factor) for s in stat]
        total = functools.reduce(jnp.add, [pltpu.roll(s, 64, 1) * c for s, c in zip(stat, scale)])
        for r in range(ranks):
            share = scale[r] / total
            for h in range(kv_heads):
                scales[r, h * each : (h + 1) * each] = jnp.broadcast_to(share[:each, h : h + 1], (each, 128))
        result = jnp.zeros((heads, head), jnp.float32)
        for r in range(ranks):
            share = scales[r]
            share = jnp.concatenate([share, share[:, : head - 128]], -1)
            result += parts[r, b].astype(jnp.float32) * share
        out[b] = result.astype(jnp.bfloat16)

    def first(b, _):
        attend(b)
        return 0

    def later(b, _):
        attend(b)
        together(b - LAG)
        return 0

    def last(b, _):
        together(b)
        return 0

    lax.fori_loop(0, LAG, first, 0)
    lax.fori_loop(LAG, sequences, later, 0)
    lax.fori_loop(sequences - LAG, sequences, last, 0)

    def drain(b, _):
        for copy in sends(b):
            copy.wait_send()
        return 0

    lax.fori_loop(0, sequences, drain, 0)


def solution(mesh):
    ranks = mesh.shape["sp"]

    def step(q, k, v):
        sequences, tokens, kv_heads, head = k.shape
        heads = q.shape[1]
        k, v = (x.transpose(0, 2, 3, 1).reshape(sequences * kv_heads, head, tokens) for x in (k, v))
        hbm = pl.BlockSpec(memory_space=pl.ANY)
        return pl.pallas_call(
            functools.partial(kernel, ranks),
            out_shape=jax.ShapeDtypeStruct(q.shape, q.dtype),
            in_specs=[hbm, hbm, hbm],
            out_specs=pl.BlockSpec(memory_space=pltpu.VMEM),
            scratch_shapes=[
                pltpu.VMEM((SLOTS, GROUP, head, tokens), k.dtype),
                pltpu.VMEM((SLOTS, GROUP, head, tokens), v.dtype),
                pltpu.VMEM(q.shape, q.dtype),
                pltpu.VMEM((heads + 8, head), jnp.float32),
                pltpu.VMEM((heads, head), jnp.float32),
                pltpu.VMEM((ranks, sequences, heads, head), jnp.bfloat16),
                pltpu.VMEM((ranks, sequences, 16, 128), jnp.float32),
                pltpu.VMEM((ranks, heads, 128), jnp.float32),
                pltpu.SemaphoreType.DMA((2, SLOTS)),
                pltpu.SemaphoreType.DMA,
                pltpu.SemaphoreType.DMA((ranks - 1, sequences)),
                pltpu.SemaphoreType.DMA((ranks, sequences)),
                pltpu.SemaphoreType.DMA((ranks - 1, sequences)),
                pltpu.SemaphoreType.DMA((ranks, sequences)),
            ],
            compiler_params=pltpu.CompilerParams(collective_id=0, has_side_effects=True, vmem_limit_bytes=42 * 2**20),
        )(q, k, v)

    return jax.shard_map(
        step,
        mesh=mesh,
        in_specs=(P("dp", None, None), P("dp", "sp", None, None), P("dp", "sp", None, None)),
        out_specs=P("dp", None, None),
        check_vma=False,
    )
```

```python
import functools

import jax
import jax.numpy as jnp
from jax import lax
from jax.experimental import pallas as pl
from jax.experimental.pallas import tpu as pltpu
from jax.sharding import PartitionSpec as P

GROUP = 4
SLOTS = 4
LAG = 3
PIECE = 16
LOG2E = 1.4426950408889634


def kernel(
    ranks, q_hbm, k_hbm, v_hbm, out, keys, values, queries, whole, weights, marks, seen, parts, stats, scales, k_sem, v_sem, q_sem, tail_sem, part_send, part_recv, stat_send, stat_recv, piece_send, piece_recv
):
    me = lax.axis_index("sp")
    sequences, heads, head = q_hbm.shape
    kv_heads = k_hbm.shape[0] // sequences
    each = heads // kv_heads
    per = kv_heads // GROUP
    rows = GROUP * each
    units = sequences * per
    factor = head**-0.5 * LOG2E
    others = [lax.rem(me + d, ranks) for d in (2, 1, 3)]
    final = sequences - 1

    def fetch(hbm, buffer, sem, unit):
        slot = lax.rem(unit, SLOTS)
        return pltpu.make_async_copy(hbm.at[pl.ds(unit * GROUP, GROUP)], buffer.at[slot], sem.at[slot])

    fetch_k = functools.partial(fetch, k_hbm, keys, k_sem)
    fetch_v = functools.partial(fetch, v_hbm, values, v_sem)

    def fetch_tail(g):
        return pltpu.make_async_copy(v_hbm.at[(units - 1) * GROUP + g], values.at[(units - 1) % SLOTS, g], tail_sem.at[g])

    q_copy = pltpu.make_async_copy(q_hbm, queries, q_sem)
    q_copy.start()
    for unit in range(SLOTS):
        fetch_k(unit).start()
        fetch_v(unit).start()

    barrier = pltpu.get_barrier_semaphore()
    for other in others:
        pl.semaphore_signal(barrier, inc=1, device_id={"sp": other})
    whole[...] = jnp.zeros_like(whole)
    q_copy.wait()

    def send(buffer, owner, b, to, send_sem, recv_sem):
        place = buffer.at[owner, b]
        return pltpu.make_async_remote_copy(place, place, send_sem, recv_sem.at[owner, b], device_id={"sp": to})

    def send_part(owner, b, d):
        return send(parts, owner, b, others[d], part_send.at[d, b], part_recv)

    def send_stat(owner, b, d):
        return send(stats, owner, b, others[d], stat_send.at[d, b], stat_recv)

    def send_piece(owner, n, d):
        first, size = (0, rows) if n == 0 else (rows + (n - 1) * PIECE, PIECE)
        place = parts.at[owner, final, pl.ds(first, size)]
        return pltpu.make_async_remote_copy(place, place, piece_send.at[d, n], piece_recv.at[owner, n], device_id={"sp": others[d]})

    pieces = 1 + (heads - rows) // PIECE
    lane = lax.broadcasted_iota(jnp.int32, (16, 128), 1)

    def load_queries(b):
        whole[:heads] = queries[b].astype(jnp.float32)

    def weigh(slot, part):
        mark = jnp.zeros((16, 128), jnp.float32) if part == 0 else marks[...]
        for g in range(GROUP):
            h = part * GROUP + g
            query = whole[h * each : h * each + 16].astype(jnp.bfloat16)
            scores = jnp.dot(query, keys[slot, g], preferred_element_type=jnp.float32)
            high = jnp.max(scores, -1, keepdims=True)
            weight = jnp.exp2((scores - high) * factor)
            total = jnp.sum(weight, -1, keepdims=True)
            mark = jnp.where(lane == h, high, mark)
            mark = jnp.where(lane == 64 + h, total, mark)
            weights[part, g] = weight.astype(jnp.bfloat16)
        marks[...] = mark

    def weighted(slot, part, g, first, size):
        a, b = weights[part, g, :, first : first + size], values[slot, g, :, first : first + size]
        return lax.dot_general(a, b, (((1,), (1,)), ((), ())), preferred_element_type=jnp.float32)

    def keep(part, g, result):
        row = (part * GROUP + g) * each
        seen[row : row + each] = result[:each]

    def gather(slot, part, g):
        keep(part, g, weighted(slot, part, g, 0, values.shape[-1]))

    def pack(b, first, size):
        parts[me, b, first : first + size] = seen[first : first + size].astype(jnp.bfloat16)

    def shares(b):
        stat = [stats[r, b] for r in range(ranks)]
        high = functools.reduce(jnp.maximum, stat)
        scale = [jnp.exp2((s - high) * factor) for s in stat]
        total = functools.reduce(jnp.add, [pltpu.roll(s, 64, 1) * c for s, c in zip(stat, scale)])
        for r in range(ranks):
            share = scale[r] / total
            for h in range(kv_heads):
                scales[r, h * each : (h + 1) * each] = jnp.broadcast_to(share[:each, h : h + 1], (each, 128))

    def combine(b, first, size):
        place = slice(first, first + size)
        result = jnp.zeros((size, head), jnp.float32)
        for r in range(ranks):
            share = scales[r, place]
            share = jnp.concatenate([share, share[:, : head - 128]], -1)
            result += parts[r, b, place].astype(jnp.float32) * share
        out[b, place] = result.astype(jnp.bfloat16)

    def arrive(b):
        for d, other in enumerate(others):
            send_part(me, b, d).wait_send()
            send_stat(me, b, d).wait_send()
            send_part(other, b, d).wait_recv()
            send_stat(other, b, d).wait_recv()

    def together(b):
        shares(b)
        combine(b, 0, heads)

    def start(copy, unit):
        @pl.when(unit < units)
        def _():
            copy(unit).start()

    def start_v(unit):
        @pl.when(unit < units - 1)
        def _():
            fetch_v(unit).start()

        @pl.when(unit == units - 1)
        def _():
            for g in range(GROUP):
                fetch_tail(g).start()

    def turn(b, part, lag):
        unit = b * per + part
        after = (part + 1) % per
        fetch_k(unit + 1).wait()
        fetch_v(unit).wait()
        if part == 0 and lag:
            arrive(b - lag)
        if after == 0:
            load_queries(b + 1)
        weigh(lax.rem(unit + 1, SLOTS), after)
        slot = lax.rem(unit, SLOTS)
        for g in range(GROUP):
            gather(slot, part, g)
        if part == 0 and lag:
            together(b - lag)
        start(fetch_k, unit + 1 + SLOTS)
        start_v(unit + SLOTS)

    def attend(b, lag):
        turn(b, 0, lag)
        stats[me, b] = marks[...]
        turn(b, 1, 0)
        pack(b, 0, heads)
        for d in range(ranks - 1):
            send_part(me, b, d).start()
            send_stat(me, b, d).start()

    load_queries(0)
    fetch_k(0).wait()
    weigh(0, 0)
    start(fetch_k, SLOTS)
    pl.semaphore_wait(barrier, ranks - 1)

    def early(b, _):
        attend(b, 0)
        return 0

    def later(b, _):
        attend(b, LAG)
        return 0

    lax.fori_loop(0, LAG, early, 0)
    lax.fori_loop(LAG, final, later, 0)

    turn(final, 0, LAG)
    stats[me, final] = marks[...]
    pack(final, 0, rows)
    for d in range(ranks - 1):
        send_stat(me, final, d).start()
        send_piece(me, 0, d).start()
    sent = 1
    half = values.shape[-1] // 2
    waiting = None
    for g in range(GROUP + 1):
        if g < GROUP:
            fetch_tail(g).wait()
            result = sum(weighted((units - 1) % SLOTS, 1, g, first, half) for first in (0, half))
        if g > 0:
            keep(1, g - 1, waiting)
        waiting = result
        while sent < pieces and rows + sent * PIECE <= rows + g * each:
            pack(final, rows + (sent - 1) * PIECE, PIECE)
            for d in range(ranks - 1):
                send_piece(me, sent, d).start()
            sent += 1
    for b in range(final - LAG + 1, final):
        arrive(b)
        together(b)
    for d, other in enumerate(others):
        send_stat(me, final, d).wait_send()
        send_stat(other, final, d).wait_recv()
    shares(final)
    for n in range(pieces):
        for d, other in enumerate(others):
            send_piece(other, n, d).wait_recv()
        if n == 0:
            combine(final, 0, rows)
        else:
            combine(final, rows + (n - 1) * PIECE, PIECE)
    for n in range(pieces):
        for d in range(ranks - 1):
            send_piece(me, n, d).wait_send()


def solution(mesh):
    ranks = mesh.shape["sp"]

    def step(q, k, v):
        sequences, tokens, kv_heads, head = k.shape
        heads = q.shape[1]
        k, v = (x.transpose(0, 2, 3, 1).reshape(sequences * kv_heads, head, tokens) for x in (k, v))
        hbm = pl.BlockSpec(memory_space=pltpu.HBM)
        dma = pltpu.SemaphoreType.DMA
        pieces = 1 + (heads - GROUP * heads // kv_heads) // PIECE
        return pl.pallas_call(
            functools.partial(kernel, ranks),
            out_shape=jax.ShapeDtypeStruct(q.shape, q.dtype),
            in_specs=[hbm, hbm, hbm],
            out_specs=pl.BlockSpec(memory_space=pltpu.VMEM),
            scratch_shapes=[
                pltpu.VMEM((SLOTS, GROUP, head, tokens), k.dtype),
                pltpu.VMEM((SLOTS, GROUP, head, tokens), v.dtype),
                pltpu.VMEM(q.shape, q.dtype),
                pltpu.VMEM((heads + 8, head), jnp.float32),
                pltpu.VMEM((2, GROUP, 16, tokens), jnp.bfloat16),
                pltpu.VMEM((16, 128), jnp.float32),
                pltpu.VMEM((heads, head), jnp.float32),
                pltpu.VMEM((ranks, sequences, heads, head), jnp.bfloat16),
                pltpu.VMEM((ranks, sequences, 16, 128), jnp.float32),
                pltpu.VMEM((ranks, heads, 128), jnp.float32),
                dma((SLOTS,)),
                dma((SLOTS,)),
                dma,
                dma((GROUP,)),
                dma((ranks - 1, sequences)),
                dma((ranks, sequences)),
                dma((ranks - 1, sequences)),
                dma((ranks, sequences)),
                dma((ranks - 1, pieces)),
                dma((ranks, pieces)),
            ],
            compiler_params=pltpu.CompilerParams(collective_id=0, has_side_effects=True, vmem_limit_bytes=42 * 2**20),
        )(pltpu.with_memory_space_constraint(q, pltpu.HBM), k, v)

    return jax.shard_map(
        step,
        mesh=mesh,
        in_specs=(P("dp", None, None), P("dp", "sp", None, None), P("dp", "sp", None, None)),
        out_specs=P("dp", None, None),
        check_vma=False,
    )
```

```python
import functools

import jax
import jax.numpy as jnp
from jax import lax
from jax.experimental import pallas as pl
from jax.experimental.pallas import tpu as pltpu
from jax.sharding import PartitionSpec as P

GROUP = 4
SLOTS = 4
LAG = 2
RING = 2 * LAG
PIECE = 16
LOG2E = 1.4426950408889634


def kernel(
    ranks, q_hbm, k_hbm, v_hbm, out, keys, values, queries, whole, weights, marks, seen, parts, stats, scales, k_sem, v_sem, q_sem, tail_sem, part_send, part_recv, stat_send, stat_recv, piece_recv
):
    me = lax.axis_index("sp")
    sequences, heads, head = q_hbm.shape
    kv_heads = k_hbm.shape[0] // sequences
    each = heads // kv_heads
    per = kv_heads // GROUP
    rows = GROUP * each
    units = sequences * per
    factor = head**-0.5 * LOG2E
    others = [lax.rem(me + d, ranks) for d in (2, 1, 3)]
    final = sequences - 1

    def fetch(hbm, buffer, sem, unit):
        slot = lax.rem(unit, SLOTS)
        return pltpu.make_async_copy(hbm.at[pl.ds(unit * GROUP, GROUP)], buffer.at[slot], sem.at[slot])

    fetch_k = functools.partial(fetch, k_hbm, keys, k_sem)
    fetch_v = functools.partial(fetch, v_hbm, values, v_sem)

    def fetch_tail(g):
        return pltpu.make_async_copy(v_hbm.at[(units - 1) * GROUP + g], values.at[(units - 1) % SLOTS, g], tail_sem.at[g])

    q_copy = pltpu.make_async_copy(q_hbm, queries, q_sem)
    q_copy.start()
    for unit in range(SLOTS):
        fetch_k(unit).start()
        fetch_v(unit).start()

    barrier = pltpu.get_barrier_semaphore()
    for other in others:
        pl.semaphore_signal(barrier, inc=1, device_id={"sp": other})
    whole[...] = jnp.zeros_like(whole)
    q_copy.wait()

    def send(buffer, owner, b, d, send_sem, recv_sem):
        place, turn = buffer.at[owner, b], lax.rem(b, RING)
        return pltpu.make_async_remote_copy(place, place, send_sem, recv_sem.at[turn], device_id={"sp": others[d]})

    def send_part(owner, b, d):
        return send(parts, owner, b, d, part_send, part_recv)

    def send_stat(owner, b, d):
        return send(stats, owner, b, d, stat_send, stat_recv)

    def piece_rows(n):
        return (0, rows) if n == 0 else (rows + (n - 1) * PIECE, PIECE)

    def send_piece(owner, n, d):
        first, size = piece_rows(n)
        place = parts.at[owner, final, pl.ds(first, size)]
        return pltpu.make_async_remote_copy(place, place, part_send, piece_recv.at[n], device_id={"sp": others[d]})

    pieces = 1 + (heads - rows) // PIECE
    lane = lax.broadcasted_iota(jnp.int32, (16, 128), 1)

    def load_queries(b):
        whole[:heads] = queries[b].astype(jnp.float32)

    def weigh(slot, part):
        mark = jnp.zeros((16, 128), jnp.float32) if part == 0 else marks[...]
        for g in range(GROUP):
            h = part * GROUP + g
            query = whole[h * each : h * each + 16].astype(jnp.bfloat16)
            scores = jnp.dot(query, keys[slot, g], preferred_element_type=jnp.float32)
            high = jnp.max(scores, -1, keepdims=True)
            weight = jnp.exp2((scores - high) * factor)
            total = jnp.sum(weight, -1, keepdims=True)
            mark = jnp.where(lane == h, high, mark)
            mark = jnp.where(lane == 64 + h, total, mark)
            weights[part, g] = weight.astype(jnp.bfloat16)
        marks[...] = mark

    def weighted(slot, part, g, first, size):
        a, b = weights[part, g, :, first : first + size], values[slot, g, :, first : first + size]
        return lax.dot_general(a, b, (((1,), (1,)), ((), ())), preferred_element_type=jnp.float32)

    def keep(part, g, result):
        row = (part * GROUP + g) * each
        seen[row : row + each] = result[:each]

    def gather(slot, part, g):
        keep(part, g, weighted(slot, part, g, 0, values.shape[-1]))

    def pack(b, first, size):
        parts[me, b, first : first + size] = seen[first : first + size].astype(jnp.bfloat16)

    def shares(b):
        stat = [stats[r, b] for r in range(ranks)]
        high = functools.reduce(jnp.maximum, stat)
        scale = [jnp.exp2((s - high) * factor) for s in stat]
        total = functools.reduce(jnp.add, [pltpu.roll(s, 64, 1) * c for s, c in zip(stat, scale)])
        for r in range(ranks):
            share = scale[r] / total
            for h in range(kv_heads):
                scales[r, h * each : (h + 1) * each] = jnp.broadcast_to(share[:each, h : h + 1], (each, 128))

    def combine(b, first, size):
        place = slice(first, first + size)
        result = jnp.zeros((size, head), jnp.float32)
        for r in range(ranks):
            share = scales[r, place]
            share = jnp.concatenate([share, share[:, : head - 128]], -1)
            result += parts[r, b, place].astype(jnp.float32) * share
        out[b, place] = result.astype(jnp.bfloat16)

    def arrive(buffer, sem, *place):
        theirs = buffer.at[(pl.ds(0, ranks - 1), *place)]
        pltpu.make_async_copy(theirs, theirs, sem).wait()

    def arrive_all(b):
        arrive(parts, part_recv.at[lax.rem(b, RING)], b)
        arrive(stats, stat_recv.at[lax.rem(b, RING)], b)

    def together(b):
        shares(b)
        combine(b, 0, heads)

    def start(copy, unit):
        @pl.when(unit < units)
        def _():
            copy(unit).start()

    def start_v(unit):
        @pl.when(unit < units - 1)
        def _():
            fetch_v(unit).start()

        @pl.when(unit == units - 1)
        def _():
            for g in range(GROUP):
                fetch_tail(g).start()

    def turn(b, part, lag):
        unit = b * per + part
        after = (part + 1) % per
        fetch_k(unit + 1).wait()
        fetch_v(unit).wait()
        if lag:
            arrive_all(b - lag)
        if after == 0:
            load_queries(b + 1)
        weigh(lax.rem(unit + 1, SLOTS), after)
        slot = lax.rem(unit, SLOTS)
        for g in range(GROUP):
            gather(slot, part, g)
        if lag:
            together(b - lag)
        start(fetch_k, unit + 1 + SLOTS)
        start_v(unit + SLOTS)

    def attend(b, lag):
        turn(b, 0, 0)
        stats[me, b] = marks[...]
        turn(b, 1, lag)
        pack(b, 0, heads)
        for d in range(ranks - 1):
            send_part(me, b, d).start()
            send_stat(me, b, d).start()

    load_queries(0)
    fetch_k(0).wait()
    weigh(0, 0)
    start(fetch_k, SLOTS)
    pl.semaphore_wait(barrier, ranks - 1)

    def early(b, _):
        attend(b, 0)
        return 0

    def later(b, _):
        attend(b, LAG)
        return 0

    lax.fori_loop(0, LAG, early, 0)
    lax.fori_loop(LAG, final, later, 0)

    turn(final, 0, LAG)
    stats[me, final] = marks[...]
    pack(final, 0, rows)
    for d in range(ranks - 1):
        send_stat(me, final, d).start()
        send_piece(me, 0, d).start()
    sent = 1
    half = values.shape[-1] // 2
    waiting = None
    for g in range(GROUP + 1):
        if g < GROUP:
            fetch_tail(g).wait()
            result = sum(weighted((units - 1) % SLOTS, 1, g, first, half) for first in (0, half))
        if g > 0:
            keep(1, g - 1, waiting)
        waiting = result
        while sent < pieces and rows + sent * PIECE <= rows + g * each:
            pack(final, rows + (sent - 1) * PIECE, PIECE)
            for d in range(ranks - 1):
                send_piece(me, sent, d).start()
            sent += 1
    for b in range(final - LAG + 1, final):
        arrive_all(b)
        together(b)
    arrive(stats, stat_recv.at[final % RING], final)
    shares(final)
    for n in range(pieces):
        first, size = piece_rows(n)
        arrive(parts, piece_recv.at[n], final, pl.ds(first, size))
        combine(final, first, size)
    arrive(parts, part_send)
    arrive(stats, stat_send)


def solution(mesh):
    ranks = mesh.shape["sp"]

    def step(q, k, v):
        sequences, tokens, kv_heads, head = k.shape
        heads = q.shape[1]
        k, v = (x.transpose(0, 2, 3, 1).reshape(sequences * kv_heads, head, tokens) for x in (k, v))
        hbm = pl.BlockSpec(memory_space=pltpu.HBM)
        dma = pltpu.SemaphoreType.DMA
        pieces = 1 + (heads - GROUP * heads // kv_heads) // PIECE
        return pl.pallas_call(
            functools.partial(kernel, ranks),
            out_shape=jax.ShapeDtypeStruct(q.shape, q.dtype),
            in_specs=[hbm, hbm, hbm],
            out_specs=pl.BlockSpec(memory_space=pltpu.VMEM),
            scratch_shapes=[
                pltpu.VMEM((SLOTS, GROUP, head, tokens), k.dtype),
                pltpu.VMEM((SLOTS, GROUP, head, tokens), v.dtype),
                pltpu.VMEM(q.shape, q.dtype),
                pltpu.VMEM((heads + 8, head), jnp.float32),
                pltpu.VMEM((2, GROUP, 16, tokens), jnp.bfloat16),
                pltpu.VMEM((16, 128), jnp.float32),
                pltpu.VMEM((heads, head), jnp.float32),
                pltpu.VMEM((ranks, sequences, heads, head), jnp.bfloat16),
                pltpu.VMEM((ranks, sequences, 16, 128), jnp.float32),
                pltpu.VMEM((ranks, heads, 128), jnp.float32),
                dma((SLOTS,)),
                dma((SLOTS,)),
                dma,
                dma((GROUP,)),
                dma,
                dma((RING,)),
                dma,
                dma((RING,)),
                dma((pieces,)),
            ],
            compiler_params=pltpu.CompilerParams(collective_id=0, has_side_effects=True, vmem_limit_bytes=42 * 2**20),
        )(pltpu.with_memory_space_constraint(q, pltpu.HBM), k, v)

    return jax.shard_map(
        step,
        mesh=mesh,
        in_specs=(P("dp", None, None), P("dp", "sp", None, None), P("dp", "sp", None, None)),
        out_specs=P("dp", None, None),
        check_vma=False,
    )
```

```python
import functools

import jax
import jax.numpy as jnp
from jax import lax
from jax.experimental import pallas as pl
from jax.experimental.pallas import tpu as pltpu
from jax.sharding import PartitionSpec as P

GROUP = 4
SLOTS = 4
LAG = 2
RING = 2 * LAG + 1
PIECE = 32
PACKED = PIECE * 3 // 2
LOG2E = 1.4426950408889634


def kernel(
    ranks, q_hbm, k_hbm, v_hbm, out, keys, values, queries, whole, weights, marks, seen, parts, stats, scales, k_sem, v_sem, q_sem, tail_sem, part_send, part_recv, stat_send, stat_recv, piece_recv
):
    me = lax.axis_index("sp")
    sequences, heads, head = q_hbm.shape
    kv_heads = k_hbm.shape[0] // sequences
    each = heads // kv_heads
    per = kv_heads // GROUP
    half = GROUP // 2
    pieces = heads // PIECE
    units = sequences * per
    factor = head**-0.5 * LOG2E
    others = [lax.rem(me + d, ranks) for d in (2, 1, 3)]
    final = sequences - 1

    def fetch(hbm, buffer, sem, unit):
        slot = lax.rem(unit, SLOTS)
        return pltpu.make_async_copy(hbm.at[pl.ds(unit * GROUP, GROUP)], buffer.at[slot], sem.at[slot])

    fetch_k = functools.partial(fetch, k_hbm, keys, k_sem)
    fetch_v = functools.partial(fetch, v_hbm, values, v_sem)

    def fetch_tail(n):
        unit, first = (units - per) + n // 2, n % 2 * half
        return pltpu.make_async_copy(v_hbm.at[pl.ds(unit * GROUP + first, half)], values.at[unit % SLOTS, pl.ds(first, half)], tail_sem.at[n])

    q_copy = pltpu.make_async_copy(q_hbm, queries, q_sem)
    q_copy.start()
    fetch_k(0).start()

    def fill(unit, _):
        fetch_v(unit - 1).start()
        fetch_k(unit).start()
        return 0

    lax.fori_loop(1, SLOTS, fill, 0)
    fetch_v(SLOTS - 1).start()

    barrier = pltpu.get_barrier_semaphore()
    for other in others:
        pl.semaphore_signal(barrier, inc=1, device_id={"sp": other})
    whole[...] = jnp.zeros_like(whole)
    q_copy.wait()

    def send(place, send_sem, recv_sem):
        for other in others:
            pltpu.make_async_remote_copy(place, place, send_sem, recv_sem, device_id={"sp": other}).start()

    def send_stat(b):
        send(stats.at[me, b], stat_send, stat_recv.at[lax.rem(b, RING)])

    def send_part(b, first, size, recv_sem):
        for p in range(first, first + size):
            pack(b, p)
        send(parts.at[me, b, pl.ds(first * PACKED, size * PACKED)], part_send, recv_sem)

    lane = lax.broadcasted_iota(jnp.int32, (8, 128), 1)
    lane16 = lax.broadcasted_iota(jnp.int32, (PIECE // 2, 128), 1)

    def load_queries(b):
        whole[:heads] = queries[b].astype(jnp.float32)

    def weigh(slot, part, between):
        scores = []
        for g in range(GROUP):
            row = (part * GROUP + g) * each
            query = whole[row : row + 16].astype(jnp.bfloat16)
            scores.append(jnp.dot(query, keys[slot, g], preferred_element_type=jnp.float32))
        between()
        mark = jnp.zeros((8, 128), jnp.float32) if part == 0 else marks[...]
        for g in range(GROUP):
            h = part * GROUP + g
            high = jnp.max(scores[g], -1, keepdims=True)
            weight = jnp.exp2((scores[g] - high) * factor)
            total = jnp.sum(weight, -1, keepdims=True)
            for at, value in ((h, high), (64 + h, total)):
                mark = jnp.where(lane == at, value[:8], mark)
                mark = jnp.where(lane == at + 8, value[8:], mark)
            weights[part, g] = weight.astype(jnp.bfloat16)
        marks[...] = mark

    def gather(slot, part, g):
        row = (part * GROUP + g) * each
        result = lax.dot_general(weights[part, g], values[slot, g], (((1,), (1,)), ((), ())), preferred_element_type=jnp.float32)
        seen[row : row + each] = result[:each]

    def pack(b, p):
        rows = seen[p * PIECE : (p + 1) * PIECE]
        rest = jnp.concatenate([rows[: PIECE // 2, 128:], rows[PIECE // 2 :, 128:]], -1)
        parts[me, b, p * PACKED : p * PACKED + PIECE] = rows[:, :128].astype(jnp.bfloat16)
        parts[me, b, p * PACKED + PIECE : (p + 1) * PACKED] = rest.astype(jnp.bfloat16)

    def shares(b):
        stat = [stats[r, b] for r in range(ranks)]
        high = functools.reduce(jnp.maximum, stat)
        scale = [jnp.exp2((s - high) * factor) for s in stat]
        total = functools.reduce(jnp.add, [pltpu.roll(s, 64, 1) * c for s, c in zip(stat, scale)])
        for r in range(ranks):
            share = scale[r] / total
            for h in range(kv_heads):
                row = h * each
                scales[r, row : row + 8] = jnp.broadcast_to(share[:, h : h + 1], (8, 128))
                scales[r, row + 8 : row + each] = jnp.broadcast_to(share[: each - 8, h + 8 : h + 9], (each - 8, 128))

    def combine(b, p):
        left = right = None
        for r in range(ranks):
            share = scales[r, p * PIECE : (p + 1) * PIECE]
            both = jnp.where(lane16 < 64, share[: PIECE // 2], share[PIECE // 2 :])
            one = parts[r, b, p * PACKED : p * PACKED + PIECE].astype(jnp.float32) * share
            two = parts[r, b, p * PACKED + PIECE : (p + 1) * PACKED].astype(jnp.float32) * both
            left, right = (one, two) if r == 0 else (left + one, right + two)
        row = p * PIECE
        out[b, row : row + PIECE, :128] = left.astype(jnp.bfloat16)
        right = right.astype(jnp.bfloat16)
        out[b, row : row + PIECE // 2, 128:] = right[:, :64]
        out[b, row + PIECE // 2 : row + PIECE, 128:] = right[:, 64:]

    def arrive(buffer, sem, *place):
        theirs = buffer.at[(pl.ds(0, ranks - 1), *place)]
        pltpu.make_async_copy(theirs, theirs, sem).wait()

    def arrive_all(b):
        arrive(parts, part_recv.at[lax.rem(b, RING)], b)
        arrive(stats, stat_recv.at[lax.rem(b, RING)], b)

    def together(b):
        shares(b)
        for p in range(pieces):
            combine(b, p)

    def start(copy, unit):
        @pl.when(unit < units)
        def _():
            copy(unit).start()

    def start_v(unit):
        @pl.when(unit < units - per)
        def _():
            fetch_v(unit).start()

        for part in range(per):

            @pl.when(unit == units - per + part)
            def _():
                for n in (0, 1):
                    fetch_tail(2 * part + n).start()

    def turn(b, part, lag):
        unit = b * per + part
        after = (part + 1) % per
        fetch_k(unit + 1).wait()
        if after == 0:
            load_queries(b + 1)

        def between():
            fetch_v(unit).wait()
            if lag:
                arrive_all(b - lag)

        weigh(lax.rem(unit + 1, SLOTS), after, between)
        slot = lax.rem(unit, SLOTS)
        for g in range(GROUP):
            gather(slot, part, g)
        if lag:
            together(b - lag)
        start(fetch_k, unit + 1 + SLOTS)
        start_v(unit + SLOTS)

    def attend(b, lag):
        recv = part_recv.at[lax.rem(b, RING)]
        turn(b, 0, 0)
        stats[me, b] = marks[...]
        send_stat(b)
        send_part(b, 0, 1, recv)
        turn(b, 1, lag)
        send_part(b, 1, pieces - 1, recv)

    load_queries(0)
    fetch_k(0).wait()
    weigh(0, 0, lambda: None)
    start(fetch_k, SLOTS)
    pl.semaphore_wait(barrier, ranks - 1)

    def early(b, _):
        attend(b, 0)
        return 0

    def later(b, _):
        attend(b, LAG)
        return 0

    lax.fori_loop(0, LAG, early, 0)
    lax.fori_loop(LAG, final, later, 0)

    slots = [(units - per + part) % SLOTS for part in range(per)]
    fetch_k(units - 1).wait()

    def between():
        fetch_tail(0).wait()
        arrive_all(final - LAG)

    weigh(slots[1], 1, between)
    for g in range(half):
        gather(slots[0], 0, g)
    stats[me, final] = marks[...]
    send_stat(final)
    for n in range(1, 4):
        fetch_tail(n).wait()
        for g in range(half):
            gather(slots[n // 2], n // 2, n % 2 * half + g)
        send_part(final, n - 1, 1, piece_recv.at[n - 1])
    together(final - LAG)
    for b in range(final - LAG + 1, final):
        arrive_all(b)
        together(b)
    arrive(stats, stat_recv.at[final % RING], final)
    shares(final)
    for p in range(pieces):
        arrive(parts, piece_recv.at[p], final, pl.ds(p * PACKED, PACKED))
        combine(final, p)
    arrive(parts, part_send)
    arrive(stats, stat_send)


def solution(mesh):
    ranks = mesh.shape["sp"]

    def step(q, k, v):
        sequences, tokens, kv_heads, head = k.shape
        heads = q.shape[1]
        k, v = (x.transpose(0, 2, 3, 1).reshape(sequences * kv_heads, head, tokens) for x in (k, v))
        hbm = pl.BlockSpec(memory_space=pltpu.HBM)
        dma = pltpu.SemaphoreType.DMA
        return pl.pallas_call(
            functools.partial(kernel, ranks),
            out_shape=jax.ShapeDtypeStruct(q.shape, q.dtype),
            in_specs=[hbm, hbm, hbm],
            out_specs=pl.BlockSpec(memory_space=pltpu.VMEM),
            scratch_shapes=[
                pltpu.VMEM((SLOTS, GROUP, head, tokens), k.dtype),
                pltpu.VMEM((SLOTS, GROUP, head, tokens), v.dtype),
                pltpu.VMEM(q.shape, q.dtype),
                pltpu.VMEM((heads + 8, head), jnp.float32),
                pltpu.VMEM((2, GROUP, 16, tokens), jnp.bfloat16),
                pltpu.VMEM((8, 128), jnp.float32),
                pltpu.VMEM((heads, head), jnp.float32),
                pltpu.VMEM((ranks, sequences, heads // PIECE * PACKED, 128), jnp.bfloat16),
                pltpu.VMEM((ranks, sequences, 8, 128), jnp.float32),
                pltpu.VMEM((ranks, heads, 128), jnp.float32),
                dma((SLOTS,)),
                dma((SLOTS,)),
                dma,
                dma((4,)),
                dma,
                dma((RING,)),
                dma,
                dma((RING,)),
                dma((heads // PIECE,)),
            ],
            compiler_params=pltpu.CompilerParams(collective_id=0, has_side_effects=True, vmem_limit_bytes=42 * 2**20),
        )(pltpu.with_memory_space_constraint(q, pltpu.HBM), k, v)

    return jax.shard_map(
        step,
        mesh=mesh,
        in_specs=(P("dp", None, None), P("dp", "sp", None, None), P("dp", "sp", None, None)),
        out_specs=P("dp", None, None),
        check_vma=False,
    )
```

```python
import functools

import jax
import jax.numpy as jnp
from jax import lax
from jax.experimental import pallas as pl
from jax.experimental.pallas import tpu as pltpu
from jax.sharding import PartitionSpec as P

GROUP = 4
SLOTS = 4
LAG = 2
RING = 2 * LAG + 1
PIECE = 32
PACKED = PIECE * 3 // 2
LOG2E = 1.4426950408889634


def kernel(
    ranks, q_hbm, k_hbm, v_hbm, out, keys, values, queries, whole, weights, marks, seen, parts, stats, scales, k_sem, v_sem, q_sem, tail_sem, part_send, part_recv, stat_send, stat_recv, piece_recv
):
    me = lax.axis_index("sp")
    sequences, heads, head = q_hbm.shape
    kv_heads = k_hbm.shape[0] // sequences
    each = heads // kv_heads
    per = kv_heads // GROUP
    half = GROUP // 2
    pieces = heads // PIECE
    units = sequences * per
    factor = head**-0.5 * LOG2E
    others = [lax.rem(me + d, ranks) for d in (2, 1, 3)]
    final = sequences - 1

    def fetch(hbm, buffer, sem, unit):
        slot = lax.rem(unit, SLOTS)
        return pltpu.make_async_copy(hbm.at[pl.ds(unit * GROUP, GROUP)], buffer.at[slot], sem.at[slot])

    fetch_k = functools.partial(fetch, k_hbm, keys, k_sem)
    fetch_v = functools.partial(fetch, v_hbm, values, v_sem)

    def fetch_tail(n):
        unit, first = (units - per) + n // 2, n % 2 * half
        return pltpu.make_async_copy(v_hbm.at[pl.ds(unit * GROUP + first, half)], values.at[unit % SLOTS, pl.ds(first, half)], tail_sem.at[n])

    q_copy = pltpu.make_async_copy(q_hbm, queries, q_sem)
    q_copy.start()
    fetch_k(0).start()

    def fill(unit, _):
        fetch_v(unit - 1).start()
        fetch_k(unit).start()
        return 0

    lax.fori_loop(1, SLOTS, fill, 0)
    fetch_v(SLOTS - 1).start()

    barrier = pltpu.get_barrier_semaphore()
    for other in others:
        pl.semaphore_signal(barrier, inc=1, device_id={"sp": other})
    whole[...] = jnp.zeros_like(whole)
    q_copy.wait()

    def send(place, send_sem, recv_sem):
        for other in others:
            pltpu.make_async_remote_copy(place, place, send_sem, recv_sem, device_id={"sp": other}).start()

    def send_stat(b):
        send(stats.at[me, b], stat_send, stat_recv.at[lax.rem(b, RING)])

    def send_part(b, first, size, recv_sem):
        for p in range(first, first + size):
            pack(b, p)
        send(parts.at[me, b, pl.ds(first * PACKED, size * PACKED)], part_send, recv_sem)

    lane = lax.broadcasted_iota(jnp.int32, (8, 128), 1)
    lane16 = lax.broadcasted_iota(jnp.int32, (PIECE // 2, 128), 1)

    def load_queries(b):
        whole[:heads] = queries[b].astype(jnp.float32)

    def weigh(slot, part, between):
        scores = []
        for g in range(GROUP):
            row = (part * GROUP + g) * each
            query = whole[row : row + 16].astype(jnp.bfloat16)
            scores.append(jnp.dot(query, keys[slot, g], preferred_element_type=jnp.float32))
        between()
        mark = jnp.zeros((8, 128), jnp.float32) if part == 0 else marks[...]
        for g in range(GROUP):
            h = part * GROUP + g
            high = jnp.max(scores[g], -1, keepdims=True)
            weight = jnp.exp2((scores[g] - high) * factor)
            total = jnp.sum(weight, -1, keepdims=True)
            for at, value in ((h, high), (64 + h, total)):
                mark = jnp.where(lane == at, value[:8], mark)
                mark = jnp.where(lane == at + 8, value[8:], mark)
            weights[part, g] = weight.astype(jnp.bfloat16)
        marks[...] = mark

    def weighted(slot, part, g):
        return lax.dot_general(weights[part, g], values[slot, g], (((1,), (1,)), ((), ())), preferred_element_type=jnp.float32)

    def keep(part, g, result):
        row = (part * GROUP + g) * each
        seen[row : row + each] = result[:each]

    def gather(slot, part, g):
        keep(part, g, weighted(slot, part, g))

    def pack(b, p):
        rows = seen[p * PIECE : (p + 1) * PIECE]
        rest = jnp.concatenate([rows[: PIECE // 2, 128:], rows[PIECE // 2 :, 128:]], -1)
        parts[me, b, p * PACKED : p * PACKED + PIECE] = rows[:, :128].astype(jnp.bfloat16)
        parts[me, b, p * PACKED + PIECE : (p + 1) * PACKED] = rest.astype(jnp.bfloat16)

    def shares(b):
        stat = [stats[r, b] for r in range(ranks)]
        high = functools.reduce(jnp.maximum, stat)
        scale = [jnp.exp2((s - high) * factor) for s in stat]
        total = functools.reduce(jnp.add, [pltpu.roll(s, 64, 1) * c for s, c in zip(stat, scale)])
        for r in range(ranks):
            share = scale[r] / total
            for h in range(kv_heads):
                row = h * each
                scales[r, row : row + 8] = jnp.broadcast_to(share[:, h : h + 1], (8, 128))
                scales[r, row + 8 : row + each] = jnp.broadcast_to(share[: each - 8, h + 8 : h + 9], (each - 8, 128))

    def combine(b, p):
        left = right = None
        for r in range(ranks):
            share = scales[r, p * PIECE : (p + 1) * PIECE]
            both = jnp.where(lane16 < 64, share[: PIECE // 2], share[PIECE // 2 :])
            one = parts[r, b, p * PACKED : p * PACKED + PIECE].astype(jnp.float32) * share
            two = parts[r, b, p * PACKED + PIECE : (p + 1) * PACKED].astype(jnp.float32) * both
            left, right = (one, two) if r == 0 else (left + one, right + two)
        row = p * PIECE
        out[b, row : row + PIECE, :128] = left.astype(jnp.bfloat16)
        right = right.astype(jnp.bfloat16)
        out[b, row : row + PIECE // 2, 128:] = right[:, :64]
        out[b, row + PIECE // 2 : row + PIECE, 128:] = right[:, 64:]

    def arrive(buffer, sem, *place):
        theirs = buffer.at[(pl.ds(0, ranks - 1), *place)]
        pltpu.make_async_copy(theirs, theirs, sem).wait()

    def arrive_all(b):
        arrive(parts, part_recv.at[lax.rem(b, RING)], b)
        arrive(stats, stat_recv.at[lax.rem(b, RING)], b)

    def together(b):
        shares(b)
        for p in range(pieces):
            combine(b, p)

    def start(copy, unit):
        @pl.when(unit < units)
        def _():
            copy(unit).start()

    def start_v(unit):
        @pl.when(unit < units - per)
        def _():
            fetch_v(unit).start()

        for part in range(per):

            @pl.when(unit == units - per + part)
            def _():
                for n in (0, 1):
                    fetch_tail(2 * part + n).start()

    def turn(b, part, lag):
        unit = b * per + part
        after = (part + 1) % per
        fetch_k(unit + 1).wait()
        if after == 0:
            load_queries(b + 1)

        def between():
            fetch_v(unit).wait()
            if lag:
                arrive_all(b - lag)

        weigh(lax.rem(unit + 1, SLOTS), after, between)
        slot = lax.rem(unit, SLOTS)
        for g in range(GROUP):
            gather(slot, part, g)
        if lag:
            together(b - lag)
        start(fetch_k, unit + 1 + SLOTS)
        start_v(unit + SLOTS)

    def attend(b, lag):
        recv = part_recv.at[lax.rem(b, RING)]
        turn(b, 0, 0)
        stats[me, b] = marks[...]
        send_stat(b)
        send_part(b, 0, 1, recv)
        turn(b, 1, lag)
        send_part(b, 1, pieces - 1, recv)

    load_queries(0)
    fetch_k(0).wait()
    weigh(0, 0, lambda: None)
    start(fetch_k, SLOTS)
    pl.semaphore_wait(barrier, ranks - 1)

    def early(b, _):
        attend(b, 0)
        return 0

    def later(b, _):
        attend(b, LAG)
        return 0

    lax.fori_loop(0, LAG, early, 0)
    lax.fori_loop(LAG, final, later, 0)

    slots = [(units - per + part) % SLOTS for part in range(per)]
    fetch_k(units - 1).wait()

    def between():
        fetch_tail(0).wait()
        arrive_all(final - LAG)

    weigh(slots[1], 1, between)
    for g in range(half):
        gather(slots[0], 0, g)
    stats[me, final] = marks[...]
    send_stat(final)
    held = None
    for n in range(1, 5):
        if n < 4:
            fetch_tail(n).wait()
            results = [weighted(slots[n // 2], n // 2, n % 2 * half + g) for g in range(half)]
        if held is not None:
            m = n - 1
            for g in range(half):
                keep(m // 2, m % 2 * half + g, held[g])
            send_part(final, m - 1, 1, piece_recv.at[m - 1])
        held = results
    together(final - LAG)
    for b in range(final - LAG + 1, final):
        arrive_all(b)
        together(b)
    arrive(stats, stat_recv.at[final % RING], final)
    shares(final)
    for p in range(pieces):
        arrive(parts, piece_recv.at[p], final, pl.ds(p * PACKED, PACKED))
        combine(final, p)
    arrive(parts, part_send)
    arrive(stats, stat_send)


def solution(mesh):
    ranks = mesh.shape["sp"]

    def step(q, k, v):
        sequences, tokens, kv_heads, head = k.shape
        heads = q.shape[1]
        k, v = (x.transpose(0, 2, 3, 1).reshape(sequences * kv_heads, head, tokens) for x in (k, v))
        hbm = pl.BlockSpec(memory_space=pltpu.HBM)
        dma = pltpu.SemaphoreType.DMA
        return pl.pallas_call(
            functools.partial(kernel, ranks),
            out_shape=jax.ShapeDtypeStruct(q.shape, q.dtype),
            in_specs=[hbm, hbm, hbm],
            out_specs=pl.BlockSpec(memory_space=pltpu.VMEM),
            scratch_shapes=[
                pltpu.VMEM((SLOTS, GROUP, head, tokens), k.dtype),
                pltpu.VMEM((SLOTS, GROUP, head, tokens), v.dtype),
                pltpu.VMEM(q.shape, q.dtype),
                pltpu.VMEM((heads + 8, head), jnp.float32),
                pltpu.VMEM((2, GROUP, 16, tokens), jnp.bfloat16),
                pltpu.VMEM((8, 128), jnp.float32),
                pltpu.VMEM((heads, head), jnp.float32),
                pltpu.VMEM((ranks, sequences, heads // PIECE * PACKED, 128), jnp.bfloat16),
                pltpu.VMEM((ranks, sequences, 8, 128), jnp.float32),
                pltpu.VMEM((ranks, heads, 128), jnp.float32),
                dma((SLOTS,)),
                dma((SLOTS,)),
                dma,
                dma((4,)),
                dma,
                dma((RING,)),
                dma,
                dma((RING,)),
                dma((heads // PIECE,)),
            ],
            compiler_params=pltpu.CompilerParams(collective_id=0, has_side_effects=True, vmem_limit_bytes=42 * 2**20),
        )(pltpu.with_memory_space_constraint(q, pltpu.HBM), k, v)

    return jax.shard_map(
        step,
        mesh=mesh,
        in_specs=(P("dp", None, None), P("dp", "sp", None, None), P("dp", "sp", None, None)),
        out_specs=P("dp", None, None),
        check_vma=False,
    )
```

```python
import functools

import jax
import jax.numpy as jnp
from jax import lax
from jax.experimental import pallas as pl
from jax.experimental.pallas import tpu as pltpu
from jax.sharding import PartitionSpec as P

GROUP = 4
SLOTS = 4
LAG = 2
RING = 2 * LAG + 1
PIECE = 32
PACKED = PIECE * 3 // 2
LOG2E = 1.4426950408889634


def kernel(
    ranks, q_hbm, k_hbm, v_hbm, out, keys, values, queries, whole, weights, marks, seen, parts, stats, scales, k_sem, v_sem, q_sem, tail_sem, part_send, part_recv, stat_send, stat_recv, piece_recv
):
    me = lax.axis_index("sp")
    sequences, heads, head = q_hbm.shape
    kv_heads = k_hbm.shape[0] // sequences
    each = heads // kv_heads
    per = kv_heads // GROUP
    half = GROUP // 2
    pieces = heads // PIECE
    units = sequences * per
    factor = head**-0.5 * LOG2E
    others = [lax.rem(me + d, ranks) for d in (2, 1, 3)]
    final = sequences - 1

    def fetch(hbm, buffer, sem, unit):
        slot = lax.rem(unit, SLOTS)
        return pltpu.make_async_copy(hbm.at[pl.ds(unit * GROUP, GROUP)], buffer.at[slot], sem.at[slot])

    fetch_k = functools.partial(fetch, k_hbm, keys, k_sem)
    fetch_v = functools.partial(fetch, v_hbm, values, v_sem)

    def fetch_tail(n):
        unit, first = (units - per) + n // 2, n % 2 * half
        return pltpu.make_async_copy(v_hbm.at[pl.ds(unit * GROUP + first, half)], values.at[unit % SLOTS, pl.ds(first, half)], tail_sem.at[n])

    q_copy = pltpu.make_async_copy(q_hbm, queries, q_sem)
    q_copy.start()
    fetch_k(0).start()

    def fill(unit, _):
        fetch_v(unit - 1).start()
        fetch_k(unit).start()
        return 0

    lax.fori_loop(1, SLOTS, fill, 0)
    fetch_v(SLOTS - 1).start()

    barrier = pltpu.get_barrier_semaphore()
    for other in others:
        pl.semaphore_signal(barrier, inc=1, device_id={"sp": other})
    whole[...] = jnp.zeros_like(whole)
    q_copy.wait()

    def send(place, send_sem, recv_sem):
        for other in others:
            pltpu.make_async_remote_copy(place, place, send_sem, recv_sem, device_id={"sp": other}).start()

    def send_stat(b):
        send(stats.at[me, b], stat_send, stat_recv.at[lax.rem(b, RING)])

    def send_pieces(b, first, size, recv_sem):
        send(parts.at[me, b, pl.ds(first * PACKED, size * PACKED)], part_send, recv_sem)

    def send_part(b, first, size, recv_sem):
        for p in range(first, first + size):
            pack(b, p)
        send_pieces(b, first, size, recv_sem)

    lane = lax.broadcasted_iota(jnp.int32, (8, 128), 1)
    lane16 = lax.broadcasted_iota(jnp.int32, (PIECE // 2, 128), 1)

    def load_queries(b):
        whole[:heads] = queries[b].astype(jnp.float32)

    def weigh(slot, part, between, beside=lambda: None):
        scores = []
        for g in range(GROUP):
            row = (part * GROUP + g) * each
            query = whole[row : row + 16].astype(jnp.bfloat16)
            scores.append(jnp.dot(query, keys[slot, g], preferred_element_type=jnp.float32))
        beside()
        between()
        mark = jnp.zeros((8, 128), jnp.float32) if part == 0 else marks[...]
        for g in range(GROUP):
            h = part * GROUP + g
            high = jnp.max(scores[g], -1, keepdims=True)
            weight = jnp.exp2((scores[g] - high) * factor)
            total = jnp.sum(weight, -1, keepdims=True)
            for at, value in ((h, high), (64 + h, total)):
                mark = jnp.where(lane == at, value[:8], mark)
                mark = jnp.where(lane == at + 8, value[8:], mark)
            weights[part, g] = weight.astype(jnp.bfloat16)
        marks[...] = mark

    def weighted(slot, part, g):
        return lax.dot_general(weights[part, g], values[slot, g], (((1,), (1,)), ((), ())), preferred_element_type=jnp.float32)

    def keep(part, g, result):
        row = (part * GROUP + g) * each
        seen[row : row + each] = result[:each]

    def gather(slot, part, g):
        keep(part, g, weighted(slot, part, g))

    def pack(b, p):
        rows = seen[p * PIECE : (p + 1) * PIECE]
        rest = jnp.concatenate([rows[: PIECE // 2, 128:], rows[PIECE // 2 :, 128:]], -1)
        parts[me, b, p * PACKED : p * PACKED + PIECE] = rows[:, :128].astype(jnp.bfloat16)
        parts[me, b, p * PACKED + PIECE : (p + 1) * PACKED] = rest.astype(jnp.bfloat16)

    def shares(b):
        stat = [stats[r, b] for r in range(ranks)]
        high = functools.reduce(jnp.maximum, stat)
        scale = [jnp.exp2((s - high) * factor) for s in stat]
        total = functools.reduce(jnp.add, [pltpu.roll(s, 64, 1) * c for s, c in zip(stat, scale)])
        for r in range(ranks):
            share = scale[r] / total
            for h in range(kv_heads):
                row = h * each
                scales[r, row : row + 8] = jnp.broadcast_to(share[:, h : h + 1], (8, 128))
                scales[r, row + 8 : row + each] = jnp.broadcast_to(share[: each - 8, h + 8 : h + 9], (each - 8, 128))

    def combine(b, p):
        left = right = None
        for r in range(ranks):
            share = scales[r, p * PIECE : (p + 1) * PIECE]
            both = jnp.where(lane16 < 64, share[: PIECE // 2], share[PIECE // 2 :])
            one = parts[r, b, p * PACKED : p * PACKED + PIECE].astype(jnp.float32) * share
            two = parts[r, b, p * PACKED + PIECE : (p + 1) * PACKED].astype(jnp.float32) * both
            left, right = (one, two) if r == 0 else (left + one, right + two)
        row = p * PIECE
        out[b, row : row + PIECE, :128] = left.astype(jnp.bfloat16)
        right = right.astype(jnp.bfloat16)
        out[b, row : row + PIECE // 2, 128:] = right[:, :64]
        out[b, row + PIECE // 2 : row + PIECE, 128:] = right[:, 64:]

    def arrive(buffer, sem, *place):
        theirs = buffer.at[(pl.ds(0, ranks - 1), *place)]
        pltpu.make_async_copy(theirs, theirs, sem).wait()

    def arrive_all(b):
        arrive(parts, part_recv.at[lax.rem(b, RING)], b)
        arrive(stats, stat_recv.at[lax.rem(b, RING)], b)

    def together(b):
        shares(b)
        for p in range(pieces):
            combine(b, p)

    def start(copy, unit):
        @pl.when(unit < units)
        def _():
            copy(unit).start()

    def start_v(unit):
        @pl.when(unit < units - per)
        def _():
            fetch_v(unit).start()

        for part in range(per):

            @pl.when(unit == units - per + part)
            def _():
                for n in (0, 1):
                    fetch_tail(2 * part + n).start()

    def turn(b, part, lag):
        unit = b * per + part
        after = (part + 1) % per
        fetch_k(unit + 1).wait()
        if after == 0:
            load_queries(b + 1)

        def between():
            fetch_v(unit).wait()
            if lag:
                arrive_all(b - lag)

        weigh(lax.rem(unit + 1, SLOTS), after, between)
        slot = lax.rem(unit, SLOTS)
        for g in range(GROUP):
            gather(slot, part, g)
        if lag:
            together(b - lag)
        start(fetch_k, unit + 1 + SLOTS)
        start_v(unit + SLOTS)

    def attend(b, lag, rest=True):
        recv = part_recv.at[lax.rem(b, RING)]
        turn(b, 0, 0)
        stats[me, b] = marks[...]
        send_stat(b)
        send_part(b, 0, 1, recv)
        turn(b, 1, lag)
        if rest:
            send_part(b, 1, pieces - 1, recv)

    load_queries(0)
    fetch_k(0).wait()
    weigh(0, 0, lambda: None)
    start(fetch_k, SLOTS)
    pl.semaphore_wait(barrier, ranks - 1)

    def early(b, _):
        attend(b, 0)
        return 0

    def later(b, _):
        attend(b, LAG)
        return 0

    lax.fori_loop(0, LAG, early, 0)
    lax.fori_loop(LAG, final - 1, later, 0)
    attend(final - 1, LAG, False)

    slots = [(units - per + part) % SLOTS for part in range(per)]
    fetch_k(units - 1).wait()

    def beside():
        for p in range(1, pieces):
            pack(final - 1, p)

    def between():
        fetch_tail(0).wait()
        arrive_all(final - LAG)
        send_pieces(final - 1, 1, pieces - 1, part_recv.at[(final - 1) % RING])

    weigh(slots[1], 1, between, beside)
    for g in range(half):
        gather(slots[0], 0, g)
    stats[me, final] = marks[...]
    send_stat(final)
    held = None
    for n in range(1, 5):
        if n < 4:
            fetch_tail(n).wait()
            results = [weighted(slots[n // 2], n // 2, n % 2 * half + g) for g in range(half)]
        if held is not None:
            m = n - 1
            for g in range(half):
                keep(m // 2, m % 2 * half + g, held[g])
            send_part(final, m - 1, 1, piece_recv.at[m - 1])
        held = results
    together(final - LAG)
    for b in range(final - LAG + 1, final):
        arrive_all(b)
        together(b)
    arrive(stats, stat_recv.at[final % RING], final)
    shares(final)
    for p in range(pieces):
        arrive(parts, piece_recv.at[p], final, pl.ds(p * PACKED, PACKED))
        combine(final, p)
    arrive(parts, part_send)
    arrive(stats, stat_send)


def solution(mesh):
    ranks = mesh.shape["sp"]

    def step(q, k, v):
        sequences, tokens, kv_heads, head = k.shape
        heads = q.shape[1]
        k, v = (x.transpose(0, 2, 3, 1).reshape(sequences * kv_heads, head, tokens) for x in (k, v))
        hbm = pl.BlockSpec(memory_space=pltpu.HBM)
        dma = pltpu.SemaphoreType.DMA
        return pl.pallas_call(
            functools.partial(kernel, ranks),
            out_shape=jax.ShapeDtypeStruct(q.shape, q.dtype),
            in_specs=[hbm, hbm, hbm],
            out_specs=pl.BlockSpec(memory_space=pltpu.VMEM),
            scratch_shapes=[
                pltpu.VMEM((SLOTS, GROUP, head, tokens), k.dtype),
                pltpu.VMEM((SLOTS, GROUP, head, tokens), v.dtype),
                pltpu.VMEM(q.shape, q.dtype),
                pltpu.VMEM((heads + 8, head), jnp.float32),
                pltpu.VMEM((2, GROUP, 16, tokens), jnp.bfloat16),
                pltpu.VMEM((8, 128), jnp.float32),
                pltpu.VMEM((heads, head), jnp.float32),
                pltpu.VMEM((ranks, sequences, heads // PIECE * PACKED, 128), jnp.bfloat16),
                pltpu.VMEM((ranks, sequences, 8, 128), jnp.float32),
                pltpu.VMEM((ranks, heads, 128), jnp.float32),
                dma((SLOTS,)),
                dma((SLOTS,)),
                dma,
                dma((4,)),
                dma,
                dma((RING,)),
                dma,
                dma((RING,)),
                dma((heads // PIECE,)),
            ],
            compiler_params=pltpu.CompilerParams(collective_id=0, has_side_effects=True, vmem_limit_bytes=42 * 2**20),
        )(pltpu.with_memory_space_constraint(q, pltpu.HBM), k, v)

    return jax.shard_map(
        step,
        mesh=mesh,
        in_specs=(P("dp", None, None), P("dp", "sp", None, None), P("dp", "sp", None, None)),
        out_specs=P("dp", None, None),
        check_vma=False,
    )
```

```python
import functools

import jax
import jax.numpy as jnp
from jax import lax
from jax.experimental import pallas as pl
from jax.experimental.pallas import tpu as pltpu
from jax.sharding import PartitionSpec as P

GROUP = 4
SLOTS = 3
LAG = 2
RING = 2 * LAG + 1
PIECE = 32
PACKED = PIECE * 3 // 2
LOG2E = 1.4426950408889634


def kernel(
    ranks, q_hbm, k_hbm, v_hbm, out, keys, values, queries, whole, weights, marks, seen, parts, stats, scales, k_sem, v_sem, q_sem, tail_sem, part_send, part_recv, stat_send, stat_recv, piece_recv
):
    me = lax.axis_index("sp")
    sequences, heads, head = q_hbm.shape
    kv_heads = k_hbm.shape[0] // sequences
    each = heads // kv_heads
    per = kv_heads // GROUP
    half = GROUP // 2
    pieces = heads // PIECE
    units = sequences * per
    factor = head**-0.5 * LOG2E
    others = [lax.rem(me + d, ranks) for d in (2, 1, 3)]
    final = sequences - 1

    def fetch(hbm, buffer, sem, unit):
        slot = lax.rem(unit, SLOTS)
        return pltpu.make_async_copy(hbm.at[pl.ds(unit * GROUP, GROUP)], buffer.at[slot], sem.at[slot])

    fetch_k = functools.partial(fetch, k_hbm, keys, k_sem)
    fetch_v = functools.partial(fetch, v_hbm, values, v_sem)

    def fetch_tail(n):
        unit, first = (units - per) + n // 2, n % 2 * half
        return pltpu.make_async_copy(v_hbm.at[pl.ds(unit * GROUP + first, half)], values.at[unit % SLOTS, pl.ds(first, half)], tail_sem.at[n])

    q_copy = pltpu.make_async_copy(q_hbm, queries, q_sem)
    q_copy.start()
    fetch_k(0).start()

    def fill(unit, _):
        fetch_v(unit - 1).start()
        fetch_k(unit).start()
        return 0

    lax.fori_loop(1, SLOTS, fill, 0)
    fetch_v(SLOTS - 1).start()

    barrier = pltpu.get_barrier_semaphore()
    for other in others:
        pl.semaphore_signal(barrier, inc=1, device_id={"sp": other})
    whole[...] = jnp.zeros_like(whole)
    q_copy.wait()

    def send(place, send_sem, recv_sem):
        for other in others:
            pltpu.make_async_remote_copy(place, place, send_sem, recv_sem, device_id={"sp": other}).start()

    def send_stat(b):
        send(stats.at[me, b], stat_send, stat_recv.at[lax.rem(b, RING)])

    def send_pieces(b, first, size, recv_sem):
        send(parts.at[me, b, pl.ds(first * PACKED, size * PACKED)], part_send, recv_sem)

    def send_part(b, first, size, recv_sem):
        for p in range(first, first + size):
            pack(b, p)
        send_pieces(b, first, size, recv_sem)

    lane = lax.broadcasted_iota(jnp.int32, (8, 128), 1)
    lane16 = lax.broadcasted_iota(jnp.int32, (PIECE // 2, 128), 1)

    def load_queries(b):
        whole[:heads] = queries[b].astype(jnp.float32)

    def weigh(slot, part, between, beside=lambda: None):
        scores = []
        for g in range(GROUP):
            row = (part * GROUP + g) * each
            query = whole[row : row + 16].astype(jnp.bfloat16)
            scores.append(jnp.dot(query, keys[slot, g], preferred_element_type=jnp.float32))
        beside()
        between()
        mark = jnp.zeros((8, 128), jnp.float32) if part == 0 else marks[...]
        for g in range(GROUP):
            h = part * GROUP + g
            high = jnp.max(scores[g], -1, keepdims=True)
            weight = jnp.exp2((scores[g] - high) * factor)
            total = jnp.sum(weight, -1, keepdims=True)
            for at, value in ((h, high), (64 + h, total)):
                mark = jnp.where(lane == at, value[:8], mark)
                mark = jnp.where(lane == at + 8, value[8:], mark)
            weights[part, g] = weight.astype(jnp.bfloat16)
        marks[...] = mark

    def weighted(slot, part, g):
        return lax.dot_general(weights[part, g], values[slot, g], (((1,), (1,)), ((), ())), preferred_element_type=jnp.float32)

    def keep(part, g, result):
        row = (part * GROUP + g) * each
        seen[row : row + each] = result[:each]

    def gather(slot, part, g):
        keep(part, g, weighted(slot, part, g))

    def pack(b, p):
        rows = seen[p * PIECE : (p + 1) * PIECE]
        rest = jnp.concatenate([rows[: PIECE // 2, 128:], rows[PIECE // 2 :, 128:]], -1)
        parts[me, b, p * PACKED : p * PACKED + PIECE] = rows[:, :128].astype(jnp.bfloat16)
        parts[me, b, p * PACKED + PIECE : (p + 1) * PACKED] = rest.astype(jnp.bfloat16)

    def shares(b):
        stat = [stats[r, b] for r in range(ranks)]
        high = functools.reduce(jnp.maximum, stat)
        scale = [jnp.exp2((s - high) * factor) for s in stat]
        total = functools.reduce(jnp.add, [pltpu.roll(s, 64, 1) * c for s, c in zip(stat, scale)])
        for r in range(ranks):
            share = scale[r] / total
            for h in range(kv_heads):
                row = h * each
                scales[r, row : row + 8] = jnp.broadcast_to(share[:, h : h + 1], (8, 128))
                scales[r, row + 8 : row + each] = jnp.broadcast_to(share[: each - 8, h + 8 : h + 9], (each - 8, 128))

    def combine(b, p):
        left = right = None
        for r in range(ranks):
            share = scales[r, p * PIECE : (p + 1) * PIECE]
            both = jnp.where(lane16 < 64, share[: PIECE // 2], share[PIECE // 2 :])
            one = parts[r, b, p * PACKED : p * PACKED + PIECE].astype(jnp.float32) * share
            two = parts[r, b, p * PACKED + PIECE : (p + 1) * PACKED].astype(jnp.float32) * both
            left, right = (one, two) if r == 0 else (left + one, right + two)
        row = p * PIECE
        out[b, row : row + PIECE, :128] = left.astype(jnp.bfloat16)
        right = right.astype(jnp.bfloat16)
        out[b, row : row + PIECE // 2, 128:] = right[:, :64]
        out[b, row + PIECE // 2 : row + PIECE, 128:] = right[:, 64:]

    def arrive(buffer, sem, *place):
        theirs = buffer.at[(pl.ds(0, ranks - 1), *place)]
        pltpu.make_async_copy(theirs, theirs, sem).wait()

    def arrive_all(b):
        arrive(parts, part_recv.at[lax.rem(b, RING)], b)
        arrive(stats, stat_recv.at[lax.rem(b, RING)], b)

    def together(b):
        shares(b)
        for p in range(pieces):
            combine(b, p)

    def start(copy, unit):
        @pl.when(unit < units)
        def _():
            copy(unit).start()

    def start_v(unit):
        @pl.when(unit < units - per)
        def _():
            fetch_v(unit).start()

        for part in range(per):

            @pl.when(unit == units - per + part)
            def _():
                for n in (0, 1):
                    fetch_tail(2 * part + n).start()

    def turn(b, part, lag):
        unit = b * per + part
        after = (part + 1) % per
        fetch_k(unit + 1).wait()
        if after == 0:
            load_queries(b + 1)

        def between():
            fetch_v(unit).wait()
            if lag:
                arrive_all(b - lag)

        weigh(lax.rem(unit + 1, SLOTS), after, between)
        slot = lax.rem(unit, SLOTS)
        for g in range(GROUP):
            gather(slot, part, g)
        if lag:
            together(b - lag)
        start(fetch_k, unit + 1 + SLOTS)
        start_v(unit + SLOTS)

    def attend(b, lag, rest=True):
        recv = part_recv.at[lax.rem(b, RING)]
        turn(b, 0, 0)
        stats[me, b] = marks[...]
        send_stat(b)
        send_part(b, 0, 1, recv)
        turn(b, 1, lag)
        if rest:
            send_part(b, 1, pieces - 1, recv)

    load_queries(0)
    fetch_k(0).wait()
    weigh(0, 0, lambda: None)
    start(fetch_k, SLOTS)
    pl.semaphore_wait(barrier, ranks - 1)

    def early(b, _):
        attend(b, 0)
        return 0

    def later(b, _):
        attend(b, LAG)
        return 0

    lax.fori_loop(0, LAG, early, 0)
    lax.fori_loop(LAG, final - 1, later, 0)
    attend(final - 1, LAG, False)

    slots = [(units - per + part) % SLOTS for part in range(per)]
    fetch_k(units - 1).wait()

    def beside():
        for p in range(1, pieces):
            pack(final - 1, p)

    def between():
        fetch_tail(0).wait()
        arrive_all(final - LAG)
        send_pieces(final - 1, 1, pieces - 1, part_recv.at[(final - 1) % RING])

    weigh(slots[1], 1, between, beside)
    for g in range(half):
        gather(slots[0], 0, g)
    stats[me, final] = marks[...]
    send_stat(final)
    held = None
    for n in range(1, 5):
        if n < 4:
            fetch_tail(n).wait()
            results = [weighted(slots[n // 2], n // 2, n % 2 * half + g) for g in range(half)]
        if held is not None:
            m = n - 1
            for g in range(half):
                keep(m // 2, m % 2 * half + g, held[g])
            send_part(final, m - 1, 1, piece_recv.at[m - 1])
        held = results
    together(final - LAG)
    for b in range(final - LAG + 1, final):
        arrive_all(b)
        together(b)
    arrive(stats, stat_recv.at[final % RING], final)
    shares(final)
    for p in range(pieces):
        arrive(parts, piece_recv.at[p], final, pl.ds(p * PACKED, PACKED))
        combine(final, p)
    arrive(parts, part_send)
    arrive(stats, stat_send)


def solution(mesh):
    ranks = mesh.shape["sp"]

    def step(q, k, v):
        sequences, tokens, kv_heads, head = k.shape
        heads = q.shape[1]
        k, v = (x.transpose(0, 2, 3, 1).reshape(sequences * kv_heads, head, tokens) for x in (k, v))
        hbm = pl.BlockSpec(memory_space=pltpu.HBM)
        dma = pltpu.SemaphoreType.DMA
        return pl.pallas_call(
            functools.partial(kernel, ranks),
            out_shape=jax.ShapeDtypeStruct(q.shape, q.dtype),
            in_specs=[hbm, hbm, hbm],
            out_specs=pl.BlockSpec(memory_space=pltpu.VMEM),
            scratch_shapes=[
                pltpu.VMEM((SLOTS, GROUP, head, tokens), k.dtype),
                pltpu.VMEM((SLOTS, GROUP, head, tokens), v.dtype),
                pltpu.VMEM(q.shape, q.dtype),
                pltpu.VMEM((heads + 8, head), jnp.float32),
                pltpu.VMEM((2, GROUP, 16, tokens), jnp.bfloat16),
                pltpu.VMEM((8, 128), jnp.float32),
                pltpu.VMEM((heads, head), jnp.float32),
                pltpu.VMEM((ranks, sequences, heads // PIECE * PACKED, 128), jnp.bfloat16),
                pltpu.VMEM((ranks, sequences, 8, 128), jnp.float32),
                pltpu.VMEM((ranks, heads, 128), jnp.float32),
                dma((SLOTS,)),
                dma((SLOTS,)),
                dma,
                dma((4,)),
                dma,
                dma((RING,)),
                dma,
                dma((RING,)),
                dma((heads // PIECE,)),
            ],
            compiler_params=pltpu.CompilerParams(collective_id=0, has_side_effects=True, vmem_limit_bytes=42 * 2**20),
        )(pltpu.with_memory_space_constraint(q, pltpu.HBM), k, v)

    return jax.shard_map(
        step,
        mesh=mesh,
        in_specs=(P("dp", None, None), P("dp", "sp", None, None), P("dp", "sp", None, None)),
        out_specs=P("dp", None, None),
        check_vma=False,
    )
```
